256 devices in a mesh: val: 8 (over x, z_lo), pts: 32 (over z_hi, y, core).
Axes of the slice: x: 4, y: 4, z: 8 (z_hi: 4, z_lo: 2; z = z_hi * 2 + z_lo), core: 2. Of those that a mesh axis runs over, the one named last changes fastest.
Arguments:
- trial: bfloat16 [512, 16384], P('val', 'pts'), may hold values from -6 to 6
- energy_gap: float32 [512, 512], P('val', 'pts'), may hold values from 0.5 to 3.5
- orb_val: bfloat16 [512, 16384], P('val'), may hold values from -0.25 to 0.25
- orb_cond: bfloat16 [512, 16384], P('pts'), may hold values from -0.25 to 0.25
- kernel: bfloat16 [16384, 16384], P('pts', 'val'), may hold values from -0.046875 to 0.046875
Outputs:
- first_step: bfloat16 [512, 16384], P('val', 'pts')
- filtered: bfloat16 [512, 16384], P('val', 'pts')
The draws below stay inside these ranges and needn't reach their ends.
All inputs are finite; a program needn't handle non-finite values.
Results may differ from the reference program's by a relative error of at most 0.029.
Values may be sent and summed in bfloat16 or wider, within the bound.
No kernel may reach another device: no remote copies, remote signals or barrier semaphores. Data moves between devices by JAX's collectives and lax.ppermute only.
A program may use at most 64 MiB of HBM per device.

```python
import math
import jax
import jax.numpy as jnp
from jax import lax

NV = 512
NC = 512
NMU = 16384
K = 32


def block_scale(stream_key, extent, shards, low, largest):
    gain, own = 1.0, jax.random.fold_in(stream_key, 6)
    for position, shards_of in shards:
        draws = jnp.exp(jax.random.uniform(jax.random.fold_in(own, position), (shards_of,), jnp.float32, low / len(shards), largest / len(shards)))
        gain = gain * jnp.repeat(draws, extent[position] // shards_of).reshape([-1 if axis == position else 1 for axis in range(len(extent))])
    return gain


def bell_draw(rng, shape, width, bound, split=(), held_as=jnp.bfloat16):
    gain = block_scale(rng, shape, split, -0.22, 0.18) if split else 1.0
    drawn = jax.random.normal(rng, shape, jnp.float32) * width * gain
    return jnp.minimum(jnp.maximum(drawn, -bound), bound).astype(held_as)


def setup_inputs(seed: int = 0) -> dict:
    key_of = jax.random.split(jax.random.key(seed), 6)
    trial = bell_draw(key_of[0], (NV, NC * K), 1.0, 6.0, ((0, 8), (1, 32)))
    energy_gap = jnp.clip(0.5 + 3.0 * jax.random.uniform(key_of[1], (NV, NC), jnp.float32) ** block_scale(key_of[1], (NV, NC), ((0, 8), (1, 32)), -0.2, 0.2), 0.5, 3.5)
    orb_val = bell_draw(key_of[2], (NV, NMU), NV ** -0.5, 0.25, ((0, 8),))
    orb_cond = bell_draw(key_of[3], (NC, NMU), NC ** -0.5, 0.25, ((0, 32),))
    kernel = bell_draw(key_of[4], (NMU, NMU), NMU ** -0.5, 0.046875, ((0, 32), (1, 8)))
    return dict(trial=trial, energy_gap=energy_gap, orb_val=orb_val, orb_cond=orb_cond, kernel=kernel)


CENTER = 2.0
HALF_WIDTH = 1.5


def pair_table(val_cols, cond_cols):
    table = val_cols.astype(jnp.float32)[:, None, :] * cond_cols.astype(jnp.float32)[None, :, :]
    return table.reshape(val_cols.shape[0] * cond_cols.shape[0], val_cols.shape[1]).astype(jnp.bfloat16)


def coupling(trial_flat, orb_val, orb_cond, kernel):
    trial_rows = trial_flat.reshape(NV * NC, K)
    block_len = math.gcd(NMU, 512)
    block_count = NMU // block_len

    def block_pairs(number):
        offset = (number * block_len).astype(jnp.int32)
        return offset, pair_table(lax.dynamic_slice_in_dim(orb_val, offset, block_len, 1),
                                  lax.dynamic_slice_in_dim(orb_cond, offset, block_len, 1))

    def encode_block(number):
        offset, pairs = block_pairs(number)
        return lax.dot_general(trial_rows, pairs, (((0,), (0,)), ((), ())), preferred_element_type=jnp.float32)

    encoded = lax.map(encode_block, jnp.arange(block_count, dtype=jnp.int32))
    fit_coefs = jnp.transpose(encoded, (1, 0, 2)).reshape(K, NMU).astype(jnp.bfloat16)
    kernel_out = lax.dot_general(fit_coefs, kernel, (((1,), (1,)), ((), ())),
                                 preferred_element_type=jnp.float32).astype(jnp.bfloat16)

    def decode_block(total_sum, number):
        offset, pairs = block_pairs(number)
        coef_block = lax.dynamic_slice_in_dim(kernel_out, offset, block_len, 1)
        added = lax.dot_general(pairs, coef_block, (((1,), (1,)), ((), ())), preferred_element_type=jnp.float32)
        return total_sum + added, None

    decoded, unused = lax.scan(decode_block, jnp.zeros((NV * NC, K), jnp.float32),
                               jnp.arange(block_count, dtype=jnp.int32))
    return decoded.reshape(NV, NC, K)


def filter_apply(trial_flat, energy_gap, orb_val, orb_cond, kernel):
    current = trial_flat.astype(jnp.float32).reshape(NV, NC, K)
    coupled = coupling(trial_flat, orb_val, orb_cond, kernel)
    return (energy_gap[:, :, None] * current + 2.0 * coupled - CENTER * current) / HALF_WIDTH


def reference(trial, energy_gap, orb_val, orb_cond, kernel):
    first_step = filter_apply(trial, energy_gap, orb_val, orb_cond, kernel).reshape(NV, NC * K).astype(jnp.bfloat16)
    second = 2.0 * filter_apply(first_step, energy_gap, orb_val, orb_cond, kernel)
    second = second - trial.astype(jnp.float32).reshape(NV, NC, K)
    return first_step, second.reshape(NV, NC * K).astype(jnp.bfloat16)
```

```python
import functools

import jax
import jax.numpy as jnp
from jax import lax
from jax.experimental import pallas as pl
from jax.experimental.pallas import tpu as pltpu
from jax.sharding import Mesh, PartitionSpec as P

K = 32
CENTER = 2.0
HALF_WIDTH = 1.5

FINE = (("x", 4), ("zl", 2), ("zh", 4), ("y", 4), ("core", 2))
VAL = ("x", "zl")
RING = ("zh", "y")
PTS = ("zh", "y", "core")

BF16 = jnp.bfloat16
F32 = jnp.float32
VMEM = pl.BlockSpec(memory_space=pltpu.VMEM)


def swap_cores(array):
    return lax.ppermute(array, "core", [(0, 1), (1, 0)])


def exchange(array, axes):
    return lax.all_to_all(array, axes, 0, 0, tiled=True)


def cost(flops, moved):
    return pl.CostEstimate(flops=int(flops), bytes_accessed=int(moved), transcendentals=0)


def encode_tile(xt, val_tile, cond_tile, out_ref, conds, width, piece):
    cols = 256
    for first in range(0, width, cols):
        total = jnp.zeros((K, cols), F32)
        for c in range(0, conds, 4):
            part = jnp.dot(
                xt[c * K : (c + 4) * K, :],
                val_tile[:, first : first + cols],
                preferred_element_type=F32,
            )
            for i in range(4):
                total = total + part[i * K : (i + 1) * K] * cond_tile[c + i : c + i + 1, first : first + cols]
        total = total.astype(BF16)
        for start in range(0, cols, min(piece, cols)):
            at = first + start
            size = min(piece, cols)
            out_ref[at // piece, :, at % piece : at % piece + size] = total[:, start : start + size]


def encode_first(h_ref, own_ref, other_ref, val_ref, cond_ref, cond_other_ref, out_ref, xt_ref):
    rows = own_ref.shape[1]

    @pl.when(pl.program_id(0) == 0)
    def _():
        xt_ref[:rows] = own_ref[...].astype(F32).T.astype(BF16)
        xt_ref[rows:] = other_ref[...].astype(F32).T.astype(BF16)

    cond = jnp.concatenate([cond_ref[...], cond_other_ref[...]], 0).astype(F32)
    encode_tile(xt_ref, val_ref, cond, out_ref.at[0], cond.shape[0], val_ref.shape[1], out_ref.shape[3])


def stepped(xt, gap, coupled, conds):
    scale = (gap - CENTER) * (1.0 / HALF_WIDTH)
    scale = jnp.broadcast_to(scale[:, None, :], (conds, K, scale.shape[1])).reshape(xt.shape)
    return xt.astype(F32) * scale + coupled * (2.0 / HALF_WIDTH)


def encode_next(
    h_ref, part_ref, recv_ref, old_ref, gap_ref, val_ref, cond_ref, cond_other_ref, out_ref, xt_ref
):
    rows = old_ref.shape[0]
    conds = rows // K
    half = rows // 2

    @pl.when(pl.program_id(0) == 0)
    def _():
        for side in range(2):
            here = slice(side * half, (side + 1) * half)
            there = slice((1 - side) * half, (2 - side) * half)
            coupled = part_ref[here] + recv_ref[there].astype(F32)
            gap = gap_ref[side * conds // 2 : (side + 1) * conds // 2]
            xt_ref[here] = stepped(old_ref[here], gap, coupled, conds // 2).astype(BF16)

    cond = jnp.concatenate([cond_ref[...], cond_other_ref[...]], 0).astype(F32)
    encode_tile(xt_ref, val_ref, cond, out_ref.at[0], cond.shape[0], val_ref.shape[1], out_ref.shape[3])


def encode(kernel, h, whole, orb_val, cond, cond_other, blocks, width, piece):
    rows = 2 * cond.shape[0] * K
    val_count = orb_val.shape[0]

    def block(shape):
        return pl.BlockSpec(shape, lambda g, h: (0, 2 * g + h[0]))

    def fixed(shape):
        return pl.BlockSpec(shape, lambda g, h: (0,) * len(shape))

    return pl.pallas_call(
        kernel,
        grid_spec=pltpu.PrefetchScalarGridSpec(
            num_scalar_prefetch=1,
            grid=(blocks,),
            in_specs=[fixed(a.shape) for a in whole]
            + [block((val_count, width)), block((cond.shape[0], width)), block((cond.shape[0], width))],
            out_specs=[
                pl.BlockSpec((1, width // piece, K, piece), lambda g, h: (g, 0, 0, 0)),
                fixed((rows, val_count)),
            ],
        ),
        out_shape=[
            jax.ShapeDtypeStruct((blocks, width // piece, K, piece), BF16),
            jax.ShapeDtypeStruct((rows, val_count), BF16),
        ],
        compiler_params=pltpu.CompilerParams(dimension_semantics=("arbitrary",)),
        cost_estimate=cost(2 * rows * val_count * blocks * width, 4 << 20),
    )(h, *whole, orb_val, cond, cond_other)


def total_kernel(groups, in_ref, out_ref):
    copies = out_ref.shape[0]
    count = in_ref.shape[0]
    for piece in range(groups):
        total = in_ref[piece].astype(F32)
        for index in range(piece + groups, count, groups):
            total = total + in_ref[index].astype(F32)
        total = total.astype(BF16)
        for copy in range(copies):
            if groups == 1:
                out_ref[copy] = total
            else:
                out_ref[copy, piece] = total


def summed(array, groups, copies):
    shape = array.shape[1:] if groups == 1 else (groups, *array.shape[1:])
    return pl.pallas_call(
        functools.partial(total_kernel, groups),
        in_specs=[VMEM],
        out_specs=VMEM,
        out_shape=jax.ShapeDtypeStruct((copies, *shape), BF16),
        cost_estimate=cost(array.size, array.size * 2),
    )(array)


def apply_kernel(h_ref, own_ref, other_ref, kernel_ref, out_ref):
    pieces, _, piece = own_ref.shape
    width = kernel_ref.shape[1] // 4
    even = h_ref[0] == 0
    total = jnp.zeros((K, kernel_ref.shape[0]), F32)
    for q in range(pieces):
        own, other = own_ref[q].astype(F32), other_ref[q].astype(F32)
        for side in range(2):
            fit = jnp.where(even, own, other) if side == 0 else jnp.where(even, other, own)
            at = q * piece
            first = width * (2 * (at // width) + side) + at % width
            total = total + lax.dot_general(
                fit.astype(BF16),
                kernel_ref[:, first : first + piece],
                (((1,), (1,)), ((), ())),
                preferred_element_type=F32,
            )
    total = total.astype(BF16)
    for copy in range(out_ref.shape[0]):
        out_ref[copy] = total


def applied(h, own, other, kernel, copies):
    rows, cols = kernel.shape
    tile = rows // 4
    return pl.pallas_call(
        apply_kernel,
        grid_spec=pltpu.PrefetchScalarGridSpec(
            num_scalar_prefetch=1,
            grid=(rows // tile,),
            in_specs=[
                pl.BlockSpec(own.shape, lambda g, h: (0, 0, 0)),
                pl.BlockSpec(own.shape, lambda g, h: (0, 0, 0)),
                pl.BlockSpec((tile, cols), lambda g, h: (g, 0)),
            ],
            out_specs=pl.BlockSpec((copies, K, tile), lambda g, h: (0, 0, g)),
        ),
        out_shape=jax.ShapeDtypeStruct((copies, K, rows), BF16),
        compiler_params=pltpu.CompilerParams(dimension_semantics=("arbitrary",)),
        cost_estimate=cost(2 * K * rows * cols, kernel.size * 2),
    )(h, own, other, kernel)


def decode_kernel(h_ref, field_ref, val_ref, cond_ref, cond_other_ref, part_ref, send_ref):
    step = pl.program_id(0)

    @pl.when(step == 0)
    def _():
        part_ref[...] = jnp.zeros_like(part_ref)

    cond = jnp.concatenate([cond_ref[...], cond_other_ref[...]], 0).astype(F32)
    field = field_ref[0].astype(F32)
    for c in range(0, cond.shape[0], 4):
        pairs = jnp.concatenate([cond[c + i : c + i + 1, :] * field for i in range(4)], 0).astype(BF16)
        part_ref[c * K : (c + 4) * K, :] += lax.dot_general(
            pairs, val_ref[...], (((1,), (1,)), ((), ())), preferred_element_type=F32
        )

    @pl.when(step == pl.num_programs(0) - 1)
    def _():
        skipped = part_ref.shape[0] - send_ref.shape[0]
        send_ref[...] = part_ref[skipped:].astype(BF16)


def decode(h, field, orb_val, cond, cond_other, sent):
    blocks, _, width = field.shape
    rows = 2 * cond.shape[0] * K
    val_count = orb_val.shape[0]

    def block(shape):
        return pl.BlockSpec(shape, lambda g, h: (0, 2 * g + h[0]))

    def fixed(shape):
        return pl.BlockSpec(shape, lambda g, h: (0,) * len(shape))

    return pl.pallas_call(
        decode_kernel,
        grid_spec=pltpu.PrefetchScalarGridSpec(
            num_scalar_prefetch=1,
            grid=(blocks,),
            in_specs=[
                pl.BlockSpec((1, K, width), lambda g, h: (g, 0, 0)),
                block((val_count, width)),
                block((cond.shape[0], width)),
                block((cond.shape[0], width)),
            ],
            out_specs=[fixed((rows, val_count)), fixed((sent, val_count))],
        ),
        out_shape=[
            jax.ShapeDtypeStruct((rows, val_count), F32),
            jax.ShapeDtypeStruct((sent, val_count), BF16),
        ],
        compiler_params=pltpu.CompilerParams(dimension_semantics=("arbitrary",)),
        cost_estimate=cost(2 * rows * val_count * blocks * width, 4 << 20),
    )(h, field, orb_val, cond, cond_other)


def turn_kernel(xt_ref, out_ref):
    out_ref[...] = xt_ref[...].astype(F32).T.astype(BF16)


def turned(xt, rows):
    return pl.pallas_call(
        turn_kernel,
        grid=(1,),
        in_specs=[pl.BlockSpec((rows, xt.shape[1]), lambda i: (0, 0))],
        out_specs=pl.BlockSpec((xt.shape[1], rows), lambda i: (0, 0)),
        out_shape=jax.ShapeDtypeStruct((xt.shape[1], rows), BF16),
        cost_estimate=cost(rows, rows * 256),
    )(xt)


def finish_kernel(part_ref, recv_ref, xt_ref, gap_ref, trial_ref, out_ref):
    coupled = part_ref[...] + recv_ref[...].astype(F32)
    second = stepped(xt_ref[...], gap_ref[...], coupled, gap_ref.shape[0])
    out_ref[...] = (2.0 * second.T - trial_ref[...].astype(F32)).astype(BF16)


def finish(part, recv, xt, gap, trial):
    val_count, rows = trial.shape

    def top(shape):
        return pl.BlockSpec(shape, lambda i: (0, 0))

    return pl.pallas_call(
        finish_kernel,
        grid=(1,),
        in_specs=[
            top((rows, val_count)),
            top((rows, val_count)),
            top((rows, val_count)),
            top((rows // K, val_count)),
            top(trial.shape),
        ],
        out_specs=top(trial.shape),
        out_shape=jax.ShapeDtypeStruct(trial.shape, BF16),
        cost_estimate=cost(rows, rows * 256),
    )(part, recv, xt, gap, trial)


def field_of(encoded, h, kernel, sizes):
    ring = sizes["zh"] * sizes["y"]
    vals = sizes["x"] * sizes["zl"]
    piece = encoded.shape[-1]
    shares = exchange(encoded.reshape(vals * sizes["y"], K, piece), (*VAL, "y"))
    shares = exchange(summed(shares, 1, ring), RING)
    fit = summed(shares, sizes["y"], 1)[0]
    image = exchange(applied(h, fit, swap_cores(fit), kernel, vals), VAL)
    return exchange(summed(image, 1, ring), RING)


def on_device(sizes, trial, energy_gap, orb_val, orb_cond, kernel):
    width = kernel.shape[0]
    blocks = sizes["zh"] * sizes["y"]
    piece = kernel.shape[1] // 2 // sizes["y"]
    own_rows = trial.shape[1]
    h = lax.axis_index("core").astype(jnp.int32).reshape(1)
    cond_other = swap_cores(orb_cond)
    trial_other = swap_cores(trial)
    gap = energy_gap.T
    gap = jnp.concatenate([gap, swap_cores(gap)], 0)

    encoded, xt = encode(
        encode_first, h, (trial, trial_other), orb_val, orb_cond, cond_other, blocks, width, piece
    )
    field = field_of(encoded, h, kernel, sizes)
    part, sent = decode(h, field, orb_val, orb_cond, cond_other, 2 * own_rows)
    encoded, xt = encode(
        encode_next,
        h,
        (part, swap_cores(sent), xt, gap),
        orb_val,
        orb_cond,
        cond_other,
        blocks,
        width,
        piece,
    )
    first_step = turned(xt, own_rows)
    field = field_of(encoded, h, kernel, sizes)
    part, sent = decode(h, field, orb_val, orb_cond, cond_other, own_rows)
    filtered = finish(part, swap_cores(sent), xt, gap, trial)
    return first_step, filtered


def build(mesh, fine):
    split = Mesh(mesh.devices.reshape([size for _, size in fine]), [name for name, _ in fine])
    placed = (P(VAL, PTS), P(VAL, PTS), P(VAL, None), P(PTS, None), P(PTS, VAL))
    return jax.shard_map(
        functools.partial(on_device, dict(fine)),
        mesh=split,
        in_specs=placed,
        out_specs=(P(VAL, PTS), P(VAL, PTS)),
        check_vma=False,
    )


def solution(mesh):
    return build(mesh, FINE)
```

```python
import functools

import jax
import jax.numpy as jnp
from jax import lax
from jax.experimental import pallas as pl
from jax.experimental.pallas import tpu as pltpu
from jax.sharding import Mesh, PartitionSpec as P

K = 32
CENTER = 2.0
HALF_WIDTH = 1.5

FINE = (("x", 4), ("zl", 2), ("zh", 4), ("y", 4), ("core", 2))
VAL = ("x", "zl")
RING = ("zh", "y")
PTS = ("zh", "y", "core")

BF16 = jnp.bfloat16
F32 = jnp.float32
VMEM = pl.BlockSpec(memory_space=pltpu.VMEM)
VMEM_LIMIT = 16 << 20


def swap_cores(array):
    return lax.ppermute(array, "core", [(0, 1), (1, 0)])


def exchange(array, axes):
    return lax.all_to_all(array, axes, 0, 0, tiled=True)


def cost(flops, moved):
    return pl.CostEstimate(flops=int(flops), bytes_accessed=int(moved), transcendentals=0)


def call(kernel, inputs, outputs, flops, scalars=0):
    smem = pl.BlockSpec(memory_space=pltpu.SMEM)
    moved = sum(2 * a.size for a in inputs) + sum(2 * o.size for o in outputs)
    return pl.pallas_call(
        kernel,
        in_specs=[smem] * scalars + [VMEM] * (len(inputs) - scalars),
        out_specs=[VMEM] * len(outputs),
        out_shape=list(outputs),
        compiler_params=pltpu.CompilerParams(vmem_limit_bytes=VMEM_LIMIT),
        cost_estimate=cost(flops, moved),
    )(*inputs)


def shape(dims, dtype=BF16):
    return jax.ShapeDtypeStruct(tuple(dims), dtype)


def encode_points(h_ref, xt_ref, val_ref, cond_ref, cond_other_ref, out_ref, width):
    pieces, _, piece = out_ref.shape
    per_block = width // piece
    conds = 2 * cond_ref.shape[0]
    cols = min(256, piece)

    def block(g, carry):
        base = pl.multiple_of((2 * g + h_ref[0]) * width, width)
        for first in range(0, width, cols):
            at = pl.ds(pl.multiple_of(base + first, cols), cols)
            cond = jnp.concatenate([cond_ref[:, at], cond_other_ref[:, at]], 0).astype(F32)
            val = val_ref[:, at]
            total = jnp.zeros((K, cols), F32)
            for c in range(0, conds, 4):
                part = jnp.dot(xt_ref[c * K : (c + 4) * K, :], val, preferred_element_type=F32)
                for i in range(4):
                    total = total + part[i * K : (i + 1) * K] * cond[c + i : c + i + 1]
            out_ref[g * per_block + first // piece, :, first % piece : first % piece + cols] = total.astype(BF16)
        return carry

    lax.fori_loop(0, pieces // per_block, block, 0)


def encode_first(width, h_ref, own_ref, other_ref, val_ref, cond_ref, cond_other_ref, out_ref, xt_ref):
    rows = own_ref.shape[1]
    xt_ref[:rows] = own_ref[...].astype(F32).T.astype(BF16)
    xt_ref[rows:] = other_ref[...].astype(F32).T.astype(BF16)
    encode_points(h_ref, xt_ref, val_ref, cond_ref, cond_other_ref, out_ref, width)


def stepped(xt, gap, coupled):
    scale = (gap - CENTER) * (1.0 / HALF_WIDTH)
    scale = jnp.broadcast_to(scale[:, None, :], (gap.shape[0], K, gap.shape[1])).reshape(xt.shape)
    return xt.astype(F32) * scale + coupled * (2.0 / HALF_WIDTH)


def encode_next(
    width, h_ref, part_ref, recv_ref, old_ref, gap_ref, val_ref, cond_ref, cond_other_ref, out_ref, xt_ref
):
    half = old_ref.shape[0] // 2
    conds = half // K
    for side in range(2):
        here = slice(side * half, (side + 1) * half)
        there = slice((1 - side) * half, (2 - side) * half)
        coupled = part_ref[here] + recv_ref[there].astype(F32)
        gap = gap_ref[side * conds : (side + 1) * conds]
        xt_ref[here] = stepped(old_ref[here], gap, coupled).astype(BF16)
    encode_points(h_ref, xt_ref, val_ref, cond_ref, cond_other_ref, out_ref, width)


def encode(kernel, h, whole, orb_val, cond, cond_other, pieces, piece, width):
    rows = 2 * cond.shape[0] * K
    val_count, points = orb_val.shape
    return call(
        functools.partial(kernel, width),
        (h, *whole, orb_val, cond, cond_other),
        (shape((pieces, K, piece)), shape((rows, val_count))),
        rows * val_count * points,
        1,
    )


def total_kernel(in_ref, out_ref):
    total = in_ref[0].astype(F32)
    for index in range(1, in_ref.shape[0]):
        total = total + in_ref[index].astype(F32)
    total = total.astype(BF16)
    for copy in range(out_ref.shape[0]):
        out_ref[copy] = total


def summed(array, copies):
    return call(total_kernel, (array,), (shape((copies, *array.shape[1:])),), array.size)[0]


def apply_kernel(pieces, width, h_ref, own_ref, other_ref, kernel_ref, out_ref):
    piece = own_ref.shape[2]
    even = h_ref[0] == 0

    def added(ref, q):
        total = ref[q].astype(F32)
        for index in range(q + pieces, ref.shape[0], pieces):
            total = total + ref[index].astype(F32)
        return total

    total = jnp.zeros((K, kernel_ref.shape[0]), F32)
    for q in range(pieces):
        own, other = added(own_ref, q), added(other_ref, q)
        for side in range(2):
            fit = jnp.where(even, own, other) if side == 0 else jnp.where(even, other, own)
            at = q * piece
            first = width * (2 * (at // width) + side) + at % width
            total = total + lax.dot_general(
                fit.astype(BF16),
                kernel_ref[:, first : first + piece],
                (((1,), (1,)), ((), ())),
                preferred_element_type=F32,
            )
    total = total.astype(BF16)
    for copy in range(out_ref.shape[0]):
        out_ref[copy] = total


def applied(h, own, other, kernel, pieces, copies):
    rows = kernel.shape[0]
    return call(
        functools.partial(apply_kernel, pieces, rows),
        (h, own, other, kernel),
        (shape((copies, K, rows)),),
        2 * K * kernel.size,
        1,
    )[0]


def decode_kernel(h_ref, field_ref, val_ref, cond_ref, cond_other_ref, part_ref, send_ref):
    blocks, _, width = field_ref.shape
    part_ref[...] = jnp.zeros_like(part_ref)

    def block(g, carry):
        at = pl.ds(pl.multiple_of((2 * g + h_ref[0]) * width, width), width)
        cond = jnp.concatenate([cond_ref[:, at], cond_other_ref[:, at]], 0).astype(F32)
        field = field_ref[g].astype(F32)
        val = val_ref[:, at]
        for c in range(0, cond.shape[0], 4):
            pairs = jnp.concatenate([cond[c + i : c + i + 1] * field for i in range(4)], 0).astype(BF16)
            part_ref[c * K : (c + 4) * K, :] += lax.dot_general(
                pairs, val, (((1,), (1,)), ((), ())), preferred_element_type=F32
            )
        return carry

    lax.fori_loop(0, blocks, block, 0)
    send_ref[...] = part_ref[part_ref.shape[0] - send_ref.shape[0] :].astype(BF16)


def decode(h, field, orb_val, cond, cond_other, sent):
    rows = 2 * cond.shape[0] * K
    val_count, points = orb_val.shape
    return call(
        decode_kernel,
        (h, field, orb_val, cond, cond_other),
        (shape((rows, val_count), F32), shape((sent, val_count))),
        rows * val_count * points,
        1,
    )


def turn_kernel(xt_ref, out_ref):
    out_ref[...] = xt_ref[: out_ref.shape[1]].astype(F32).T.astype(BF16)


def turned(xt, rows):
    return call(turn_kernel, (xt,), (shape((xt.shape[1], rows)),), xt.size)[0]


def finish_kernel(part_ref, recv_ref, xt_ref, gap_ref, trial_ref, out_ref):
    rows = recv_ref.shape[0]
    coupled = part_ref[:rows] + recv_ref[...].astype(F32)
    second = stepped(xt_ref[:rows], gap_ref[: rows // K], coupled)
    out_ref[...] = (2.0 * second.T - trial_ref[...].astype(F32)).astype(BF16)


def finish(part, recv, xt, gap, trial):
    return call(finish_kernel, (part, recv, xt, gap, trial), (shape(trial.shape),), 8 * trial.size)[0]


def field_of(encoded, h, kernel, sizes):
    ring = sizes["zh"] * sizes["y"]
    shares = exchange(encoded, (*VAL, "y"))
    shares = exchange(summed(shares, ring), RING)
    image = applied(h, shares, swap_cores(shares), kernel, sizes["y"], sizes["x"] * sizes["zl"])
    return exchange(summed(exchange(image, VAL), ring), RING)


def on_device(sizes, trial, energy_gap, orb_val, orb_cond, kernel):
    width = kernel.shape[0]
    pieces = sizes["x"] * sizes["zl"] * sizes["y"]
    piece = kernel.shape[1] // 2 // sizes["y"]
    own_rows = trial.shape[1]
    h = lax.axis_index("core").astype(jnp.int32).reshape(1)
    cond_other = swap_cores(orb_cond)
    trial_other = swap_cores(trial)
    gap = energy_gap.T
    gap = jnp.concatenate([gap, swap_cores(gap)], 0)
    orbitals = (orb_val, orb_cond, cond_other)

    encoded, xt = encode(encode_first, h, (trial, trial_other), *orbitals, pieces, piece, width)
    field = field_of(encoded, h, kernel, sizes)
    part, sent = decode(h, field, *orbitals, 2 * own_rows)
    encoded, xt = encode(encode_next, h, (part, swap_cores(sent), xt, gap), *orbitals, pieces, piece, width)
    first_step = turned(xt, own_rows)
    field = field_of(encoded, h, kernel, sizes)
    part, sent = decode(h, field, *orbitals, own_rows)
    filtered = finish(part, swap_cores(sent), xt, gap, trial)
    return first_step, filtered


def build(mesh, fine):
    split = Mesh(mesh.devices.reshape([size for _, size in fine]), [name for name, _ in fine])
    placed = (P(VAL, PTS), P(VAL, PTS), P(VAL, None), P(PTS, None), P(PTS, VAL))
    return jax.shard_map(
        functools.partial(on_device, dict(fine)),
        mesh=split,
        in_specs=placed,
        out_specs=(P(VAL, PTS), P(VAL, PTS)),
        check_vma=False,
    )


def solution(mesh):
    return build(mesh, FINE)
```

```python
import functools

import jax
import jax.numpy as jnp
from jax import lax
from jax.experimental import pallas as pl
from jax.experimental.pallas import tpu as pltpu
from jax.sharding import Mesh, PartitionSpec as P

K = 32
CENTER = 2.0
HALF_WIDTH = 1.5

FINE = (("x", 4), ("zl", 2), ("zh", 4), ("y", 4), ("core", 2))
VAL = ("x", "zl")
RING = ("zh", "y")
PTS = ("zh", "y", "core")

BF16 = jnp.bfloat16
F32 = jnp.float32
VMEM = pl.BlockSpec(memory_space=pltpu.VMEM)
VMEM_LIMIT = 16 << 20
UNROLL = 2


def swap_cores(array):
    return lax.ppermute(array, "core", [(0, 1), (1, 0)])


def exchange(array, axes):
    return lax.all_to_all(array, axes, 0, 0, tiled=True)


def cost(flops, moved):
    return pl.CostEstimate(flops=int(flops), bytes_accessed=int(moved), transcendentals=0)


def call(kernel, inputs, outputs, flops, scalars=0):
    smem = pl.BlockSpec(memory_space=pltpu.SMEM)
    moved = sum(2 * a.size for a in inputs) + sum(2 * o.size for o in outputs)
    return pl.pallas_call(
        kernel,
        in_specs=[smem] * scalars + [VMEM] * (len(inputs) - scalars),
        out_specs=[VMEM] * len(outputs),
        out_shape=list(outputs),
        compiler_params=pltpu.CompilerParams(vmem_limit_bytes=VMEM_LIMIT),
        cost_estimate=cost(flops, moved),
    )(*inputs)


def shape(dims, dtype=BF16):
    return jax.ShapeDtypeStruct(tuple(dims), dtype)


def block_of(ref, g, h_ref, width):
    return ref[:, pl.ds(pl.multiple_of((2 * g + h_ref[0]) * width, width), width)]


def encode_points(h_ref, xt_refs, val_ref, cond_refs, out_ref, width):
    pieces, _, piece = out_ref.shape
    per_block = width // piece
    cols = min(256, piece)

    def block(g, carry):
        base = pl.multiple_of((2 * g + h_ref[0]) * width, width)
        for first in range(0, width, cols):
            at = pl.ds(pl.multiple_of(base + first, cols), cols)
            val = val_ref[:, at]
            total = jnp.zeros((K, cols), F32)
            for xt_ref, cond_ref in zip(xt_refs, cond_refs):
                cond = cond_ref[:, at].astype(F32)
                for c in range(0, cond.shape[0], 4):
                    part = jnp.dot(xt_ref[c * K : (c + 4) * K, :], val, preferred_element_type=F32)
                    for i in range(4):
                        total = total + part[i * K : (i + 1) * K] * cond[c + i : c + i + 1]
            out_ref[g * per_block + first // piece, :, first % piece : first % piece + cols] = total.astype(BF16)
        return carry

    lax.fori_loop(0, pieces // per_block, block, 0, unroll=UNROLL)


def encode_first(
    width,
    h_ref,
    own_ref,
    other_ref,
    gap_ref,
    gap_other_ref,
    val_ref,
    cond_ref,
    cond_other_ref,
    out_ref,
    xt_ref,
    xt_other_ref,
    scale_ref,
):
    conds = gap_ref.shape[0]
    scale_ref[:conds] = (gap_ref[...] - CENTER) * (1.0 / HALF_WIDTH)
    scale_ref[conds:] = (gap_other_ref[...] - CENTER) * (1.0 / HALF_WIDTH)
    xt_ref[...] = own_ref[...].astype(F32).T.astype(BF16)
    xt_other_ref[...] = other_ref[...].astype(F32).T.astype(BF16)
    encode_points(h_ref, (xt_ref, xt_other_ref), val_ref, (cond_ref, cond_other_ref), out_ref, width)


def stepped(xt, scale, coupled):
    scale = jnp.broadcast_to(scale[:, None, :], (scale.shape[0], K, scale.shape[1])).reshape(xt.shape)
    return xt.astype(F32) * scale + coupled * (2.0 / HALF_WIDTH)


def encode_next(
    width,
    h_ref,
    part_ref,
    recv_ref,
    old_ref,
    old_other_ref,
    scale_ref,
    val_ref,
    cond_ref,
    cond_other_ref,
    out_ref,
    xt_ref,
    xt_other_ref,
):
    half = old_ref.shape[0]
    conds = half // K
    for side, (old, new) in enumerate(((old_ref, xt_ref), (old_other_ref, xt_other_ref))):
        here = slice(side * half, (side + 1) * half)
        there = slice((1 - side) * half, (2 - side) * half)
        coupled = part_ref[here] + recv_ref[there].astype(F32)
        scale = scale_ref[side * conds : (side + 1) * conds]
        new[...] = stepped(old[...], scale, coupled).astype(BF16)
    encode_points(h_ref, (xt_ref, xt_other_ref), val_ref, (cond_ref, cond_other_ref), out_ref, width)


def encode(kernel, h, whole, orbitals, pieces, piece, width, *more):
    val_count, points = orbitals[0].shape
    rows = orbitals[1].shape[0] * K
    return call(
        functools.partial(kernel, width),
        (h, *whole, *orbitals),
        (shape((pieces, K, piece)), shape((rows, val_count)), shape((rows, val_count)), *more),
        2 * rows * val_count * points,
        1,
    )


def total_kernel(in_ref, out_ref):
    total = in_ref[0].astype(F32)
    for index in range(1, in_ref.shape[0]):
        total = total + in_ref[index].astype(F32)
    total = total.astype(BF16)
    for copy in range(out_ref.shape[0]):
        out_ref[copy] = total


def summed(array, copies):
    return call(total_kernel, (array,), (shape((copies, *array.shape[1:])),), array.size)[0]


def apply_kernel(pieces, width, h_ref, own_ref, other_ref, kernel_ref, out_ref):
    piece = own_ref.shape[2]
    even = h_ref[0] == 0

    def added(ref, q):
        total = ref[q].astype(F32)
        for index in range(q + pieces, ref.shape[0], pieces):
            total = total + ref[index].astype(F32)
        return total

    total = jnp.zeros((K, kernel_ref.shape[0]), F32)
    for q in range(pieces):
        own, other = added(own_ref, q), added(other_ref, q)
        for side in range(2):
            fit = jnp.where(even, own, other) if side == 0 else jnp.where(even, other, own)
            at = q * piece
            first = width * (2 * (at // width) + side) + at % width
            total = total + lax.dot_general(
                fit.astype(BF16),
                kernel_ref[:, first : first + piece],
                (((1,), (1,)), ((), ())),
                preferred_element_type=F32,
            )
    total = total.astype(BF16)
    for copy in range(out_ref.shape[0]):
        out_ref[copy] = total


def applied(h, own, other, kernel, pieces, copies):
    rows = kernel.shape[0]
    return call(
        functools.partial(apply_kernel, pieces, rows),
        (h, own, other, kernel),
        (shape((copies, K, rows)),),
        2 * K * kernel.size,
        1,
    )[0]


def stack_kernel(*refs):
    out_ref = refs[-1]
    for index, ref in enumerate(refs[:-1]):
        out_ref[index] = ref[0]


def stacked(arrays):
    return call(stack_kernel, arrays, (shape((len(arrays), *arrays[0].shape[1:])),), arrays[0].size)[0]


def decode_kernel(steps, y_step, sizes, more, h_ref, zh_ref, y_ref, field_ref, val_ref, cond_ref, cond_other_ref, *refs):
    part_ref = refs[1] if more else refs[0]
    width = field_ref.shape[2]
    y = lax.rem(y_ref[0] + sizes["y"] - y_step, sizes["y"])
    for index, z_step in enumerate(steps):
        g = lax.rem(zh_ref[0] + sizes["zh"] - z_step, sizes["zh"]) * sizes["y"] + y
        field = field_ref[index].astype(F32)
        val = block_of(val_ref, g, h_ref, width)
        row = 0
        for ref in (cond_ref, cond_other_ref):
            cond = block_of(ref, g, h_ref, width).astype(F32)
            for c in range(0, cond.shape[0], 4):
                pairs = jnp.concatenate([cond[c + i : c + i + 1] * field for i in range(4)], 0).astype(BF16)
                rows = slice(row, row + 4 * K)
                added = lax.dot_general(pairs, val, (((1,), (1,)), ((), ())), preferred_element_type=F32)
                if index == 0:
                    part_ref[rows, :] = refs[0][rows, :] + added if more else added
                else:
                    part_ref[rows, :] += added
                row += 4 * K
    if len(refs) > more + 1:
        send_ref = refs[-1]
        send_ref[...] = part_ref[part_ref.shape[0] - send_ref.shape[0] :].astype(BF16)


def behind(count):
    return sorted(range(1, count), key=lambda step: -min(step, count - step))


def shifted(array, axis, count, step):
    return lax.ppermute(array, axis, [(i, (i + step) % count) for i in range(count)])


def decode(field, place, orbitals, sizes, sent):
    val_count = orbitals[0].shape[0]
    rows = 2 * orbitals[1].shape[0] * K
    steps = [0, *behind(sizes["zh"])]
    field = stacked([field, *(shifted(field, "zh", sizes["zh"], step) for step in steps[1:])])
    far = behind(sizes["y"])
    fields = {step: shifted(field, "y", sizes["y"], step) for step in far}
    fields[0] = field
    parts = ()
    for y_step in (0, *reversed(far)):
        here = fields[y_step]
        outputs = (shape((rows, val_count), F32),)
        if y_step == far[0]:
            outputs += (shape((sent, val_count)),)
        parts = call(
            functools.partial(decode_kernel, steps, y_step, sizes, len(parts)),
            (*place, here, *orbitals, *parts),
            outputs,
            2 * rows * val_count * here.shape[0] * here.shape[2],
            len(place),
        )
    return parts


def turn_kernel(xt_ref, out_ref):
    out_ref[...] = xt_ref[...].astype(F32).T.astype(BF16)


def turned(xt):
    return call(turn_kernel, (xt,), (shape(xt.shape[::-1]),), xt.size)[0]


def finish_kernel(part_ref, recv_ref, xt_ref, scale_ref, trial_ref, out_ref):
    rows = recv_ref.shape[0]
    coupled = part_ref[:rows] + recv_ref[...].astype(F32)
    second = stepped(xt_ref[...], scale_ref[: rows // K], coupled)
    out_ref[...] = (2.0 * second.T - trial_ref[...].astype(F32)).astype(BF16)


def finish(part, recv, xt, scale, trial):
    return call(finish_kernel, (part, recv, xt, scale, trial), (shape(trial.shape),), 8 * trial.size)[0]


def field_of(encoded, h, kernel, sizes):
    ring = sizes["zh"] * sizes["y"]
    shares = exchange(encoded, (*VAL, "y"))
    shares = exchange(summed(shares, ring), RING)
    image = applied(h, shares, swap_cores(shares), kernel, sizes["y"], sizes["x"] * sizes["zl"])
    return summed(exchange(image, VAL), 1)


def on_device(sizes, trial, energy_gap, orb_val, orb_cond, kernel):
    width = kernel.shape[0]
    pieces = sizes["x"] * sizes["zl"] * sizes["y"]
    piece = kernel.shape[1] // 2 // sizes["y"]
    place = [lax.axis_index(axis).astype(jnp.int32).reshape(1) for axis in ("core", "zh", "y")]
    h = place[0]
    orbitals = (orb_val, orb_cond, swap_cores(orb_cond))
    gap = energy_gap.T
    whole = (trial, swap_cores(trial), gap, swap_cores(gap))
    scale = shape((2 * gap.shape[0], gap.shape[1]), F32)

    encoded, xt, xt_other, scale = encode(encode_first, h, whole, orbitals, pieces, piece, width, scale)
    field = field_of(encoded, h, kernel, sizes)
    part, sent = decode(field, place, orbitals, sizes, 2 * xt.shape[0])
    whole = (part, swap_cores(sent), xt, xt_other, scale)
    encoded, xt, _ = encode(encode_next, h, whole, orbitals, pieces, piece, width)
    first_step = turned(xt)
    field = field_of(encoded, h, kernel, sizes)
    part, sent = decode(field, place, orbitals, sizes, xt.shape[0])
    filtered = finish(part, swap_cores(sent), xt, scale, trial)
    return first_step, filtered


def build(mesh, fine):
    split = Mesh(mesh.devices.reshape([size for _, size in fine]), [name for name, _ in fine])
    placed = (P(VAL, PTS), P(VAL, PTS), P(VAL, None), P(PTS, None), P(PTS, VAL))
    return jax.shard_map(
        functools.partial(on_device, dict(fine)),
        mesh=split,
        in_specs=placed,
        out_specs=(P(VAL, PTS), P(VAL, PTS)),
        check_vma=False,
    )


def solution(mesh):
    return build(mesh, FINE)
```

```python
import functools

import jax
import jax.numpy as jnp
from jax import lax
from jax.experimental import pallas as pl
from jax.experimental.pallas import tpu as pltpu
from jax.sharding import Mesh, PartitionSpec as P

K = 32
CENTER = 2.0
HALF_WIDTH = 1.5

FINE = (("x", 4), ("zl", 2), ("zh", 4), ("y", 4), ("core", 2))
VAL = ("x", "zl")
RING = ("zh", "y")
PTS = ("zh", "y", "core")

BF16 = jnp.bfloat16
F32 = jnp.float32
VMEM = pl.BlockSpec(memory_space=pltpu.VMEM)
VMEM_LIMIT = 16 << 20
UNROLL = 2
START_FLOPS = 4_000_000_000


def swap_cores(array):
    return lax.ppermute(array, "core", [(0, 1), (1, 0)])


def exchange(array, axes):
    return lax.all_to_all(array, axes, 0, 0, tiled=True)


def cost(flops, moved):
    return pl.CostEstimate(flops=int(flops), bytes_accessed=int(moved), transcendentals=0)


def call(kernel, inputs, outputs, flops, scalars=0):
    smem = pl.BlockSpec(memory_space=pltpu.SMEM)
    moved = sum(2 * a.size for a in inputs) + sum(2 * o.size for o in outputs)
    return pl.pallas_call(
        kernel,
        in_specs=[smem] * scalars + [VMEM] * (len(inputs) - scalars),
        out_specs=[VMEM] * len(outputs),
        out_shape=list(outputs),
        compiler_params=pltpu.CompilerParams(vmem_limit_bytes=VMEM_LIMIT),
        cost_estimate=cost(flops, moved),
    )(*inputs)


def shape(dims, dtype=BF16):
    return jax.ShapeDtypeStruct(tuple(dims), dtype)


def block_of(ref, g, h_ref, width):
    return ref[:, pl.ds(pl.multiple_of((2 * g + h_ref[0]) * width, width), width)]


def encode_points(h_ref, xt_refs, val_ref, cond_refs, out_ref, width):
    pieces, _, piece = out_ref.shape
    per_block = width // piece
    cols = min(256, piece)

    def block(g, carry):
        base = pl.multiple_of((2 * g + h_ref[0]) * width, width)
        for first in range(0, width, cols):
            at = pl.ds(pl.multiple_of(base + first, cols), cols)
            val = val_ref[:, at]
            total = jnp.zeros((K, cols), F32)
            for xt_ref, cond_ref in zip(xt_refs, cond_refs):
                cond = cond_ref[:, at].astype(F32)
                for c in range(0, cond.shape[0], 4):
                    part = jnp.dot(xt_ref[c * K : (c + 4) * K, :], val, preferred_element_type=F32)
                    for i in range(4):
                        total = total + part[i * K : (i + 1) * K] * cond[c + i : c + i + 1]
            out_ref[g * per_block + first // piece, :, first % piece : first % piece + cols] = total.astype(BF16)
        return carry

    lax.fori_loop(0, pieces // per_block, block, 0, unroll=UNROLL)


def encode_first(width, h_ref, xt_ref, xt_other_ref, val_ref, cond_ref, cond_other_ref, out_ref):
    encode_points(h_ref, (xt_ref, xt_other_ref), val_ref, (cond_ref, cond_other_ref), out_ref, width)


def stepped(xt, scale, coupled):
    scale = jnp.broadcast_to(scale[:, None, :], (scale.shape[0], K, scale.shape[1])).reshape(xt.shape)
    return xt.astype(F32) * scale + coupled * (2.0 / HALF_WIDTH)


def encode_next(
    width,
    h_ref,
    part_ref,
    recv_ref,
    old_ref,
    old_other_ref,
    scale_ref,
    scale_other_ref,
    val_ref,
    cond_ref,
    cond_other_ref,
    out_ref,
    xt_ref,
    xt_other_ref,
):
    half = old_ref.shape[0]
    sides = ((old_ref, scale_ref, xt_ref), (old_other_ref, scale_other_ref, xt_other_ref))
    for side, (old, scale, new) in enumerate(sides):
        here = slice(side * half, (side + 1) * half)
        there = slice((1 - side) * half, (2 - side) * half)
        coupled = part_ref[here] + recv_ref[there].astype(F32)
        new[...] = stepped(old[...], scale[...], coupled).astype(BF16)
    encode_points(h_ref, (xt_ref, xt_other_ref), val_ref, (cond_ref, cond_other_ref), out_ref, width)


def encode(kernel, h, whole, orbitals, pieces, piece, width, *more):
    val_count, points = orbitals[0].shape
    rows = orbitals[1].shape[0] * K
    return call(
        functools.partial(kernel, width),
        (h, *whole, *orbitals),
        (shape((pieces, K, piece)), *more),
        2 * rows * val_count * points,
        1,
    )


def total_kernel(in_ref, out_ref):
    total = in_ref[0].astype(F32)
    for index in range(1, in_ref.shape[0]):
        total = total + in_ref[index].astype(F32)
    total = total.astype(BF16)
    for copy in range(out_ref.shape[0]):
        out_ref[copy] = total


def summed(array, copies):
    return call(total_kernel, (array,), (shape((copies, *array.shape[1:])),), array.size)[0]


def apply_kernel(pieces, width, h_ref, own_ref, other_ref, kernel_ref, out_ref):
    piece = own_ref.shape[2]
    even = h_ref[0] == 0

    def added(ref, q):
        total = ref[q].astype(F32)
        for index in range(q + pieces, ref.shape[0], pieces):
            total = total + ref[index].astype(F32)
        return total

    total = jnp.zeros((K, kernel_ref.shape[0]), F32)
    for q in range(pieces):
        own, other = added(own_ref, q), added(other_ref, q)
        for side in range(2):
            fit = jnp.where(even, own, other) if side == 0 else jnp.where(even, other, own)
            at = q * piece
            first = width * (2 * (at // width) + side) + at % width
            total = total + lax.dot_general(
                fit.astype(BF16),
                kernel_ref[:, first : first + piece],
                (((1,), (1,)), ((), ())),
                preferred_element_type=F32,
            )
    total = total.astype(BF16)
    for copy in range(out_ref.shape[0]):
        out_ref[copy] = total


def applied(h, own, other, kernel, pieces, copies):
    rows = kernel.shape[0]
    return call(
        functools.partial(apply_kernel, pieces, rows),
        (h, own, other, kernel),
        (shape((copies, K, rows)),),
        2 * K * kernel.size,
        1,
    )[0]


def stack_kernel(*refs):
    out_ref = refs[-1]
    for index, ref in enumerate(refs[:-1]):
        out_ref[index] = ref[0]


def stacked(arrays):
    return call(stack_kernel, arrays, (shape((len(arrays), *arrays[0].shape[1:])),), arrays[0].size)[0]


def decode_kernel(steps, sizes, h_ref, zh_ref, y_ref, field_ref, val_ref, cond_ref, cond_other_ref, *refs):
    *before, part_ref, send_ref = (*refs, None) if len(refs) == 1 else refs
    width = field_ref.shape[2]
    for index, z_step in enumerate(steps):
        g = lax.rem(zh_ref[0] + sizes["zh"] - z_step, sizes["zh"]) * sizes["y"] + y_ref[0]
        field = field_ref[index].astype(F32)
        val = block_of(val_ref, g, h_ref, width)
        row = 0
        for ref in (cond_ref, cond_other_ref):
            cond = block_of(ref, g, h_ref, width).astype(F32)
            for c in range(0, cond.shape[0], 4):
                pairs = jnp.concatenate([cond[c + i : c + i + 1] * field for i in range(4)], 0).astype(BF16)
                rows = slice(row, row + 4 * K)
                added = lax.dot_general(pairs, val, (((1,), (1,)), ((), ())), preferred_element_type=F32)
                if index == 0:
                    part_ref[rows, :] = before[0][rows, :] + added if before else added
                else:
                    part_ref[rows, :] += added
                row += 4 * K
    if send_ref is not None:
        send_ref[...] = part_ref[part_ref.shape[0] - send_ref.shape[0] :].astype(BF16)


def behind(count):
    return sorted(range(1, count), key=lambda step: -min(step, count - step))


def shifted(array, axis, count, step):
    return lax.ppermute(array, axis, [(i, (i + step) % count) for i in range(count)])


def decode(field, place, orbitals, sizes, sent):
    val_count = orbitals[0].shape[0]
    rows = 2 * orbitals[1].shape[0] * K
    steps = [0, *reversed(behind(sizes["zh"]))]
    field = stacked([field, *(shifted(field, "zh", sizes["zh"], step) for step in steps[1:])])
    far = behind(sizes["y"])
    fields = {step: shifted(field, "y", sizes["y"], step) for step in far}
    fields[0] = field
    h, zh, y = place
    parts = ()
    for y_step in (0, *reversed(far)):
        here = fields[y_step]
        outputs = (shape((rows, val_count), F32),)
        if y_step:
            outputs += (shape((sent, val_count)),)
        parts = call(
            functools.partial(decode_kernel, tuple(steps), sizes),
            (h, zh, lax.rem(y + (sizes["y"] - y_step), sizes["y"]), here, *orbitals, *parts[:1]),
            outputs,
            2 * rows * val_count * here.shape[0] * here.shape[2],
            len(place),
        )
    return parts


def start_kernel(trial_ref, gap_ref, xt_ref, scale_ref):
    xt_ref[...] = trial_ref[...].astype(F32).T.astype(BF16)
    scale_ref[...] = (gap_ref[...] - CENTER) * (1.0 / HALF_WIDTH)


def started(trial, gap):
    return call(start_kernel, (trial, gap), (shape(trial.shape[::-1]), shape(gap.shape, F32)), START_FLOPS)


def turn_kernel(xt_ref, out_ref):
    out_ref[...] = xt_ref[...].astype(F32).T.astype(BF16)


def turned(xt):
    return call(turn_kernel, (xt,), (shape(xt.shape[::-1]),), xt.size)[0]


def finish_kernel(part_ref, recv_ref, xt_ref, scale_ref, trial_ref, out_ref):
    rows = recv_ref.shape[0]
    coupled = part_ref[:rows] + recv_ref[...].astype(F32)
    second = stepped(xt_ref[...], scale_ref[...], coupled)
    out_ref[...] = (2.0 * second.T - trial_ref[...].astype(F32)).astype(BF16)


def finish(part, recv, xt, scale, trial):
    return call(finish_kernel, (part, recv, xt, scale, trial), (shape(trial.shape),), 8 * trial.size)[0]


def field_of(encoded, h, kernel, sizes):
    ring = sizes["zh"] * sizes["y"]
    shares = exchange(encoded, (*VAL, "y"))
    shares = exchange(summed(shares, ring), RING)
    image = applied(h, shares, swap_cores(shares), kernel, sizes["y"], sizes["x"] * sizes["zl"])
    return summed(exchange(image, VAL), 1)


def on_device(sizes, trial, energy_gap, orb_val, orb_cond, kernel):
    width = kernel.shape[0]
    pieces = sizes["x"] * sizes["zl"] * sizes["y"]
    piece = kernel.shape[1] // 2 // sizes["y"]
    place = [lax.axis_index(axis).astype(jnp.int32).reshape(1) for axis in ("core", "zh", "y")]
    h = place[0]
    orbitals = (orb_val, orb_cond, swap_cores(orb_cond))
    xt, scale = started(trial, energy_gap.T)
    xt_other, scale_other = swap_cores(xt), swap_cores(scale)

    encoded = encode(encode_first, h, (xt, xt_other), orbitals, pieces, piece, width)[0]
    field = field_of(encoded, h, kernel, sizes)
    part, sent = decode(field, place, orbitals, sizes, 2 * xt.shape[0])
    whole = (part, swap_cores(sent), xt, xt_other, scale, scale_other)
    states = (shape(xt.shape), shape(xt.shape))
    encoded, xt, _ = encode(encode_next, h, whole, orbitals, pieces, piece, width, *states)
    first_step = turned(xt)
    field = field_of(encoded, h, kernel, sizes)
    part, sent = decode(field, place, orbitals, sizes, xt.shape[0])
    filtered = finish(part, swap_cores(sent), xt, scale, trial)
    return first_step, filtered


def build(mesh, fine):
    split = Mesh(mesh.devices.reshape([size for _, size in fine]), [name for name, _ in fine])
    placed = (P(VAL, PTS), P(VAL, PTS), P(VAL, None), P(PTS, None), P(PTS, VAL))
    return jax.shard_map(
        functools.partial(on_device, dict(fine)),
        mesh=split,
        in_specs=placed,
        out_specs=(P(VAL, PTS), P(VAL, PTS)),
        check_vma=False,
    )


def solution(mesh):
    return build(mesh, FINE)
```

```python
import functools

import jax
import jax.numpy as jnp
from jax import lax
from jax.experimental import pallas as pl
from jax.experimental.pallas import tpu as pltpu
from jax.sharding import Mesh, PartitionSpec as P


K = 32
CENTER = 2.0
HALF_WIDTH = 1.5

FINE = (("x", 4), ("zl", 2), ("zh", 4), ("y", 4), ("core", 2))
VAL = ("x", "zl")
RING = ("zh", "y")
PTS = ("zh", "y", "core")

BF16 = jnp.bfloat16
F32 = jnp.float32
VMEM = pl.BlockSpec(memory_space=pltpu.VMEM)
VMEM_LIMIT = 16 << 20
UNROLL = 2
START_FLOPS = 4_000_000_000


def swap_cores(array):
    return lax.ppermute(array, "core", [(0, 1), (1, 0)])


def exchange(array, axes):
    return lax.all_to_all(array, axes, 0, 0, tiled=True)


def cost(flops, moved):
    return pl.CostEstimate(flops=int(flops), bytes_accessed=int(moved), transcendentals=0)


def call(kernel, inputs, outputs, flops, scalars=0):
    smem = pl.BlockSpec(memory_space=pltpu.SMEM)
    moved = sum(2 * a.size for a in inputs) + sum(2 * o.size for o in outputs)
    return pl.pallas_call(
        kernel,
        in_specs=[smem] * scalars + [VMEM] * (len(inputs) - scalars),
        out_specs=[VMEM] * len(outputs),
        out_shape=list(outputs),
        compiler_params=pltpu.CompilerParams(vmem_limit_bytes=VMEM_LIMIT),
        cost_estimate=cost(flops, moved),
    )(*inputs)


def shape(dims, dtype=BF16):
    return jax.ShapeDtypeStruct(tuple(dims), dtype)


def block_of(ref, g, h_ref, width):
    return ref[:, pl.ds(pl.multiple_of((2 * g + h_ref[0]) * width, width), width)]


def encode_points(h_ref, xt_refs, val_ref, cond_refs, out_ref, width):
    pieces, _, piece = out_ref.shape
    per_block = width // piece
    cols = min(256, piece)

    def block(g, carry):
        base = pl.multiple_of((2 * g + h_ref[0]) * width, width)
        for first in range(0, width, cols):
            at = pl.ds(pl.multiple_of(base + first, cols), cols)
            val = val_ref[:, at]
            total = jnp.zeros((K, cols), F32)
            for xt_ref, cond_ref in zip(xt_refs, cond_refs):
                cond = cond_ref[:, at].astype(F32)
                for c in range(0, cond.shape[0], 4):
                    part = jnp.dot(xt_ref[c * K : (c + 4) * K, :], val, preferred_element_type=F32)
                    for i in range(4):
                        total = total + part[i * K : (i + 1) * K] * cond[c + i : c + i + 1]
            out_ref[g * per_block + first // piece, :, first % piece : first % piece + cols] = total.astype(BF16)
        return carry

    lax.fori_loop(0, pieces // per_block, block, 0, unroll=UNROLL)


def encode_first(width, h_ref, xt_ref, xt_other_ref, val_ref, cond_ref, cond_other_ref, out_ref):
    encode_points(h_ref, (xt_ref, xt_other_ref), val_ref, (cond_ref, cond_other_ref), out_ref, width)


def stepped(xt, gap, coupled):
    scale = (gap - CENTER) * (1.0 / HALF_WIDTH)
    scale = jnp.broadcast_to(scale[:, None, :], (scale.shape[0], K, scale.shape[1])).reshape(xt.shape)
    return xt.astype(F32) * scale + coupled * (2.0 / HALF_WIDTH)


def encode_next(
    width,
    h_ref,
    part_ref,
    recv_ref,
    old_ref,
    old_other_ref,
    gap_ref,
    gap_other_ref,
    val_ref,
    cond_ref,
    cond_other_ref,
    out_ref,
    xt_ref,
    xt_other_ref,
):
    half = old_ref.shape[0]
    sides = ((old_ref, gap_ref, xt_ref), (old_other_ref, gap_other_ref, xt_other_ref))
    for side, (old, gap, new) in enumerate(sides):
        here = slice(side * half, (side + 1) * half)
        there = slice((1 - side) * half, (2 - side) * half)
        coupled = part_ref[here] + recv_ref[there].astype(F32)
        new[...] = stepped(old[...], gap[...], coupled).astype(BF16)
    encode_points(h_ref, (xt_ref, xt_other_ref), val_ref, (cond_ref, cond_other_ref), out_ref, width)


def encode(kernel, h, whole, orbitals, pieces, piece, width, *more):
    val_count, points = orbitals[0].shape
    rows = orbitals[1].shape[0] * K
    return call(
        functools.partial(kernel, width),
        (h, *whole, *orbitals),
        (shape((pieces, K, piece)), *more),
        2 * rows * val_count * points,
        1,
    )


def total_kernel(in_ref, out_ref):
    total = in_ref[0].astype(F32)
    for index in range(1, in_ref.shape[0]):
        total = total + in_ref[index].astype(F32)
    total = total.astype(BF16)
    for copy in range(out_ref.shape[0]):
        out_ref[copy] = total


def summed(array, copies):
    return call(total_kernel, (array,), (shape((copies, *array.shape[1:])),), array.size)[0]


def apply_kernel(pieces, width, h_ref, own_ref, other_ref, kernel_ref, out_ref):
    piece = own_ref.shape[2]
    even = h_ref[0] == 0

    def added(ref, q):
        total = ref[q].astype(F32)
        for index in range(q + pieces, ref.shape[0], pieces):
            total = total + ref[index].astype(F32)
        return total

    total = jnp.zeros((K, kernel_ref.shape[0]), F32)
    for q in range(pieces):
        own, other = added(own_ref, q), added(other_ref, q)
        for side in range(2):
            fit = jnp.where(even, own, other) if side == 0 else jnp.where(even, other, own)
            at = q * piece
            first = width * (2 * (at // width) + side) + at % width
            total = total + lax.dot_general(
                fit.astype(BF16),
                kernel_ref[:, first : first + piece],
                (((1,), (1,)), ((), ())),
                preferred_element_type=F32,
            )
    total = total.astype(BF16)
    for copy in range(out_ref.shape[0]):
        out_ref[copy] = total


def applied(h, own, other, kernel, pieces, copies):
    rows = kernel.shape[0]
    return call(
        functools.partial(apply_kernel, pieces, rows),
        (h, own, other, kernel),
        (shape((copies, K, rows)),),
        2 * K * kernel.size,
        1,
    )[0]


def stack_kernel(*refs):
    out_ref = refs[-1]
    for index, ref in enumerate(refs[:-1]):
        out_ref[index] = ref[0]


def stacked(arrays):
    return call(stack_kernel, arrays, (shape((len(arrays), *arrays[0].shape[1:])),), arrays[0].size)[0]


def decode_kernel(steps, sizes, more, h_ref, zh_ref, y_ref, field_ref, val_ref, cond_ref, cond_other_ref, *refs):
    before = refs[:more]
    part_ref, send_ref = (*refs[more:], None)[:2]
    width = field_ref.shape[2]
    for index, z_step in enumerate(steps):
        g = lax.rem(zh_ref[0] + sizes["zh"] - z_step, sizes["zh"]) * sizes["y"] + y_ref[0]
        field = field_ref[index].astype(F32)
        val = block_of(val_ref, g, h_ref, width)
        row = 0
        for ref in (cond_ref, cond_other_ref):
            cond = block_of(ref, g, h_ref, width).astype(F32)
            for c in range(0, cond.shape[0], 4):
                pairs = jnp.concatenate([cond[c + i : c + i + 1] * field for i in range(4)], 0).astype(BF16)
                rows = slice(row, row + 4 * K)
                added = lax.dot_general(pairs, val, (((1,), (1,)), ((), ())), preferred_element_type=F32)
                if index == 0:
                    part_ref[rows, :] = before[0][rows, :] + added if before else added
                else:
                    part_ref[rows, :] += added
                row += 4 * K
    if send_ref is not None:
        send_ref[...] = part_ref[part_ref.shape[0] - send_ref.shape[0] :].astype(BF16)


def behind(count):
    return sorted(range(1, count), key=lambda step: -min(step, count - step))


def shifted(array, axis, count, step):
    return lax.ppermute(array, axis, [(i, (i + step) % count) for i in range(count)])


def decode(field, place, orbitals, sizes, sent):
    val_count = orbitals[0].shape[0]
    rows = 2 * orbitals[1].shape[0] * K
    steps = [0, *behind(sizes["zh"])]
    fields = [field]
    for step in steps[1:]:
        fields.append(shifted(field, "zh", sizes["zh"], step))
    field = stacked(fields)
    far = behind(sizes["y"])
    fields = {step: shifted(field, "y", sizes["y"], step) for step in far}
    fields[0] = field
    h, zh, y = place
    parts = ()
    for y_step in (0, *reversed(far)):
        here = fields[y_step]
        outputs = (shape((rows, val_count), F32),)
        if y_step == far[0]:
            outputs += (shape((sent, val_count)),)
        parts = call(
            functools.partial(decode_kernel, tuple(steps), sizes, len(parts)),
            (h, zh, lax.rem(y + (sizes["y"] - y_step), sizes["y"]), here, *orbitals, *parts),
            outputs,
            2 * rows * val_count * here.shape[0] * here.shape[2],
            len(place),
        )
    return parts


def turn_kernel(xt_ref, out_ref):
    out_ref[...] = xt_ref[...].astype(F32).T.astype(BF16)


def turned(xt, flops):
    return call(turn_kernel, (xt,), (shape(xt.shape[::-1]),), flops)[0]


def finish_kernel(part_ref, recv_ref, xt_ref, gap_ref, trial_ref, out_ref):
    rows = recv_ref.shape[0]
    coupled = part_ref[:rows] + recv_ref[...].astype(F32)
    second = stepped(xt_ref[...], gap_ref[...], coupled)
    out_ref[...] = (2.0 * second.T - trial_ref[...].astype(F32)).astype(BF16)


def finish(part, recv, xt, gap, trial):
    return call(finish_kernel, (part, recv, xt, gap, trial), (shape(trial.shape),), 8 * trial.size)[0]


def field_of(encoded, h, kernel, sizes):
    ring = sizes["zh"] * sizes["y"]
    shares = exchange(encoded, (*VAL, "y"))
    shares = exchange(summed(shares, ring), RING)
    image = applied(h, shares, swap_cores(shares), kernel, sizes["y"], sizes["x"] * sizes["zl"])
    return summed(exchange(image, VAL), 1)


def on_device(sizes, trial, energy_gap, orb_val, orb_cond, kernel):
    width = kernel.shape[0]
    pieces = sizes["x"] * sizes["zl"] * sizes["y"]
    piece = kernel.shape[1] // 2 // sizes["y"]
    place = [lax.axis_index(axis).astype(jnp.int32).reshape(1) for axis in ("core", "zh", "y")]
    h = place[0]
    orbitals = (orb_val, orb_cond, swap_cores(orb_cond))
    gap = energy_gap.T
    xt = turned(trial, START_FLOPS)
    xt_other = swap_cores(xt)

    encoded = encode(encode_first, h, (xt, xt_other), orbitals, pieces, piece, width)[0]
    field = field_of(encoded, h, kernel, sizes)
    part, sent = decode(field, place, orbitals, sizes, 2 * xt.shape[0])
    whole = (part, swap_cores(sent), xt, xt_other, gap, swap_cores(gap))
    states = (shape(xt.shape), shape(xt.shape))
    encoded, xt, _ = encode(encode_next, h, whole, orbitals, pieces, piece, width, *states)
    first_step = turned(xt, xt.size)
    field = field_of(encoded, h, kernel, sizes)
    part, sent = decode(field, place, orbitals, sizes, xt.shape[0])
    filtered = finish(part, swap_cores(sent), xt, gap, trial)
    return first_step, filtered


def build(mesh, fine):
    split = Mesh(mesh.devices.reshape([size for _, size in fine]), [name for name, _ in fine])
    placed = (P(VAL, PTS), P(VAL, PTS), P(VAL, None), P(PTS, None), P(PTS, VAL))
    return jax.shard_map(
        functools.partial(on_device, dict(fine)),
        mesh=split,
        in_specs=placed,
        out_specs=(P(VAL, PTS), P(VAL, PTS)),
        check_vma=False,
    )


def solution(mesh):
    return build(mesh, FINE)
```

```python
import functools

import jax
import jax.numpy as jnp
from jax import lax
from jax.experimental import pallas as pl
from jax.experimental.pallas import tpu as pltpu
from jax.sharding import Mesh, PartitionSpec as P


K = 32
CENTER = 2.0
HALF_WIDTH = 1.5

FINE = (("x", 4), ("zl", 2), ("zh", 4), ("y", 4), ("core", 2))
VAL = ("x", "zl")
PTS = ("zh", "y", "core")

BF16 = jnp.bfloat16
F32 = jnp.float32
VMEM = pl.BlockSpec(memory_space=pltpu.VMEM)
VMEM_LIMIT = 16 << 20
UNROLL = 2
START_FLOPS = 4_000_000_000


def swap_cores(array):
    return lax.ppermute(array, "core", [(0, 1), (1, 0)])


def exchange(array, axes):
    return lax.all_to_all(array, axes, 0, 0, tiled=True)


def cost(flops, moved):
    return pl.CostEstimate(flops=int(flops), bytes_accessed=int(moved), transcendentals=0)


def call(kernel, inputs, outputs, flops, scalars=0):
    smem = pl.BlockSpec(memory_space=pltpu.SMEM)
    moved = sum(2 * a.size for a in inputs) + sum(2 * o.size for o in outputs)
    return pl.pallas_call(
        kernel,
        in_specs=[smem] * scalars + [VMEM] * (len(inputs) - scalars),
        out_specs=[VMEM] * len(outputs),
        out_shape=list(outputs),
        compiler_params=pltpu.CompilerParams(vmem_limit_bytes=VMEM_LIMIT),
        cost_estimate=cost(flops, moved),
    )(*inputs)


def shape(dims, dtype=BF16):
    return jax.ShapeDtypeStruct(tuple(dims), dtype)


def block_of(ref, g, h_ref, width):
    return ref[:, pl.ds(pl.multiple_of((2 * g + h_ref[0]) * width, width), width)]


def encode_points(h_ref, xt_refs, val_ref, cond_refs, out_ref, width):
    pieces, _, piece = out_ref.shape
    per_block = width // piece
    cols = min(256, piece)

    def block(g, carry):
        base = pl.multiple_of((2 * g + h_ref[0]) * width, width)
        for first in range(0, width, cols):
            at = pl.ds(pl.multiple_of(base + first, cols), cols)
            val = val_ref[:, at]
            total = jnp.zeros((K, cols), F32)
            for xt_ref, cond_ref in zip(xt_refs, cond_refs):
                cond = cond_ref[:, at].astype(F32)
                for c in range(0, cond.shape[0], 4):
                    part = jnp.dot(xt_ref[c * K : (c + 4) * K, :], val, preferred_element_type=F32)
                    for i in range(4):
                        total = total + part[i * K : (i + 1) * K] * cond[c + i : c + i + 1]
            out_ref[g * per_block + first // piece, :, first % piece : first % piece + cols] = total.astype(BF16)
        return carry

    lax.fori_loop(0, pieces // per_block, block, 0, unroll=UNROLL)


def encode_first(width, h_ref, xt_ref, xt_other_ref, val_ref, cond_ref, cond_other_ref, out_ref):
    encode_points(h_ref, (xt_ref, xt_other_ref), val_ref, (cond_ref, cond_other_ref), out_ref, width)


def stepped(xt, gap, coupled):
    scale = (gap - CENTER) * (1.0 / HALF_WIDTH)
    scale = jnp.broadcast_to(scale[:, None, :], (scale.shape[0], K, scale.shape[1])).reshape(xt.shape)
    return xt.astype(F32) * scale + coupled * (2.0 / HALF_WIDTH)


def encode_next(
    width,
    h_ref,
    part_ref,
    recv_ref,
    old_ref,
    old_other_ref,
    gap_ref,
    gap_other_ref,
    val_ref,
    cond_ref,
    cond_other_ref,
    out_ref,
    xt_ref,
    xt_other_ref,
):
    half = old_ref.shape[0]
    sides = ((old_ref, gap_ref, xt_ref), (old_other_ref, gap_other_ref, xt_other_ref))
    for side, (old, gap, new) in enumerate(sides):
        here = slice(side * half, (side + 1) * half)
        there = slice((1 - side) * half, (2 - side) * half)
        coupled = part_ref[here] + recv_ref[there].astype(F32)
        new[...] = stepped(old[...], gap[...], coupled).astype(BF16)
    encode_points(h_ref, (xt_ref, xt_other_ref), val_ref, (cond_ref, cond_other_ref), out_ref, width)


def encode(kernel, h, whole, orbitals, pieces, piece, width, *more):
    val_count, points = orbitals[0].shape
    rows = orbitals[1].shape[0] * K
    return call(
        functools.partial(kernel, width),
        (h, *whole, *orbitals),
        (shape((pieces, K, piece)), *more),
        2 * rows * val_count * points,
        1,
    )


def total_kernel(in_ref, out_ref):
    total = in_ref[0].astype(F32)
    for index in range(1, in_ref.shape[0]):
        total = total + in_ref[index].astype(F32)
    total = total.astype(BF16)
    for copy in range(out_ref.shape[0]):
        out_ref[copy] = total


def summed(array, copies):
    return call(total_kernel, (array,), (shape((copies, *array.shape[1:])),), array.size)[0]


def add_kernel(*refs):
    *parts, out_ref = refs
    total = parts[0][...].astype(F32)
    for part in parts[1:]:
        total = total + part[...].astype(F32)
    out_ref[...] = total.astype(BF16)


def added(arrays):
    return call(add_kernel, arrays, (shape(arrays[0].shape),), START_FLOPS)[0]


def apply_kernel(steps, pieces, width, h_ref, y_ref, *refs):
    *fit_refs, kernel_ref, out_ref = refs
    piece = fit_refs[0].shape[2]
    even = h_ref[0] == 0
    total = jnp.zeros((K, kernel_ref.shape[0]), F32)
    for step, ref in zip(steps, fit_refs):
        at = lax.rem(y_ref[0] + pieces - step, pieces) * piece
        first = 2 * width * lax.div(at, width) + lax.rem(at, width)
        own, other = ref[0].astype(F32), ref[1].astype(F32)
        for side in range(2):
            fit = jnp.where(even, own, other) if side == 0 else jnp.where(even, other, own)
            cols = pl.ds(pl.multiple_of(first + side * width, piece), piece)
            total = total + lax.dot_general(
                fit.astype(BF16), kernel_ref[:, cols], (((1,), (1,)), ((), ())), preferred_element_type=F32
            )
    total = total.astype(BF16)
    for copy in range(out_ref.shape[0]):
        out_ref[copy] = total


def applied(h, y, fits, steps, kernel, copies):
    rows = kernel.shape[0]
    return call(
        functools.partial(apply_kernel, tuple(steps), len(steps), rows),
        (h, y, *fits, kernel),
        (shape((copies, K, rows)),),
        2 * K * kernel.size,
        2,
    )[0]


def stack_kernel(*refs):
    out_ref = refs[-1]
    for index, ref in enumerate(refs[:-1]):
        out_ref[index] = ref[0]


def stacked(arrays):
    return call(stack_kernel, arrays, (shape((len(arrays), *arrays[0].shape[1:])),), START_FLOPS)[0]


def behind(count):
    return sorted(range(1, count), key=lambda step: -min(step, count - step))


def shifted(array, axis, count, step):
    return lax.ppermute(array, axis, [(i, (i + step) % count) for i in range(count)])


def along_zh(array, sizes):
    arrays = [array]
    for step in behind(sizes["zh"]):
        arrays.append(shifted(array, "zh", sizes["zh"], step))
    return arrays


def decode_kernel(steps, sizes, more, h_ref, zh_ref, y_ref, field_ref, val_ref, cond_ref, cond_other_ref, *refs):
    before = refs[:more]
    part_ref, send_ref = (*refs[more:], None)[:2]
    width = field_ref.shape[2]
    for index, z_step in enumerate(steps):
        g = lax.rem(zh_ref[0] + sizes["zh"] - z_step, sizes["zh"]) * sizes["y"] + y_ref[0]
        field = field_ref[index].astype(F32)
        val = block_of(val_ref, g, h_ref, width)
        row = 0
        for ref in (cond_ref, cond_other_ref):
            cond = block_of(ref, g, h_ref, width).astype(F32)
            for c in range(0, cond.shape[0], 4):
                pairs = jnp.concatenate([cond[c + i : c + i + 1] * field for i in range(4)], 0).astype(BF16)
                rows = slice(row, row + 4 * K)
                added = lax.dot_general(pairs, val, (((1,), (1,)), ((), ())), preferred_element_type=F32)
                if index == 0:
                    part_ref[rows, :] = before[0][rows, :] + added if before else added
                else:
                    part_ref[rows, :] += added
                row += 4 * K
    if send_ref is not None:
        send_ref[...] = part_ref[part_ref.shape[0] - send_ref.shape[0] :].astype(BF16)


def decode(field, place, orbitals, sizes, sent):
    val_count = orbitals[0].shape[0]
    rows = 2 * orbitals[1].shape[0] * K
    steps = [0, *behind(sizes["zh"])]
    field = stacked(along_zh(field, sizes))
    far = behind(sizes["y"])
    fields = {step: shifted(field, "y", sizes["y"], step) for step in far}
    fields[0] = field
    h, zh, y = place
    parts = ()
    for y_step in (0, *reversed(far)):
        here = fields[y_step]
        outputs = (shape((rows, val_count), F32),)
        if y_step == far[0]:
            outputs += (shape((sent, val_count)),)
        parts = call(
            functools.partial(decode_kernel, tuple(steps), sizes, len(parts)),
            (h, zh, lax.rem(y + (sizes["y"] - y_step), sizes["y"]), here, *orbitals, *parts),
            outputs,
            2 * rows * val_count * here.shape[0] * here.shape[2],
            len(place),
        )
    return parts


def turn_kernel(xt_ref, out_ref):
    out_ref[...] = xt_ref[...].astype(F32).T.astype(BF16)


def turned(xt, flops):
    return call(turn_kernel, (xt,), (shape(xt.shape[::-1]),), flops)[0]


def finish_kernel(part_ref, recv_ref, xt_ref, gap_ref, trial_ref, out_ref):
    rows = recv_ref.shape[0]
    coupled = part_ref[:rows] + recv_ref[...].astype(F32)
    second = stepped(xt_ref[...], gap_ref[...], coupled)
    out_ref[...] = (2.0 * second.T - trial_ref[...].astype(F32)).astype(BF16)


def finish(part, recv, xt, gap, trial):
    return call(finish_kernel, (part, recv, xt, gap, trial), (shape(trial.shape),), 8 * trial.size)[0]


def field_of(encoded, place, kernel, sizes):
    h, _, y = place
    fit = added(along_zh(summed(exchange(encoded, (*VAL, "y")), 1), sizes))
    fit = stacked([fit, swap_cores(fit)])
    steps = [0, *behind(sizes["y"])]
    fits = [fit, *(shifted(fit, "y", sizes["y"], step) for step in steps[1:])]
    image = applied(h, y, fits, steps, kernel, sizes["x"] * sizes["zl"])
    return summed(exchange(image, VAL), 1)


def on_device(sizes, trial, energy_gap, orb_val, orb_cond, kernel):
    width = kernel.shape[0]
    pieces = sizes["x"] * sizes["zl"] * sizes["y"]
    piece = kernel.shape[1] // 2 // sizes["y"]
    place = [lax.axis_index(axis).astype(jnp.int32).reshape(1) for axis in ("core", "zh", "y")]
    h = place[0]
    orbitals = (orb_val, orb_cond, swap_cores(orb_cond))
    gap = energy_gap.T
    xt = turned(trial, START_FLOPS)
    xt_other = swap_cores(xt)

    encoded = encode(encode_first, h, (xt, xt_other), orbitals, pieces, piece, width)[0]
    field = field_of(encoded, place, kernel, sizes)
    part, sent = decode(field, place, orbitals, sizes, 2 * xt.shape[0])
    whole = (part, swap_cores(sent), xt, xt_other, gap, swap_cores(gap))
    states = (shape(xt.shape), shape(xt.shape))
    encoded, xt, _ = encode(encode_next, h, whole, orbitals, pieces, piece, width, *states)
    first_step = turned(xt, xt.size)
    field = field_of(encoded, place, kernel, sizes)
    part, sent = decode(field, place, orbitals, sizes, xt.shape[0])
    filtered = finish(part, swap_cores(sent), xt, gap, trial)
    return first_step, filtered


def build(mesh, fine):
    split = Mesh(mesh.devices.reshape([size for _, size in fine]), [name for name, _ in fine])
    placed = (P(VAL, PTS), P(VAL, PTS), P(VAL, None), P(PTS, None), P(PTS, VAL))
    return jax.shard_map(
        functools.partial(on_device, dict(fine)),
        mesh=split,
        in_specs=placed,
        out_specs=(P(VAL, PTS), P(VAL, PTS)),
        check_vma=False,
    )


def solution(mesh):
    return build(mesh, FINE)
```

```python
import functools

import jax
import jax.numpy as jnp
from jax import lax
from jax.experimental import pallas as pl
from jax.experimental.pallas import tpu as pltpu
from jax.sharding import Mesh, PartitionSpec as P


K = 32
CENTER = 2.0
HALF_WIDTH = 1.5

FINE = (("x", 4), ("zl", 2), ("zh", 4), ("y", 4), ("core", 2))
VAL = ("x", "zl")
RING = ("y", "zh")
PTS = ("zh", "y", "core")

BF16 = jnp.bfloat16
F32 = jnp.float32
VMEM = pl.BlockSpec(memory_space=pltpu.VMEM)
VMEM_LIMIT = 16 << 20
UNROLL = 4
START_FLOPS = 4_000_000_000


def swap_cores(array):
    return lax.ppermute(array, "core", [(0, 1), (1, 0)])


def exchange(array, axes):
    return lax.all_to_all(array, axes, 0, 0, tiled=True)


def cost(flops, moved):
    return pl.CostEstimate(flops=int(flops), bytes_accessed=int(moved), transcendentals=0)


def call(kernel, inputs, outputs, flops, scalars=0):
    smem = pl.BlockSpec(memory_space=pltpu.SMEM)
    moved = sum(2 * a.size for a in inputs) + sum(2 * o.size for o in outputs)
    return pl.pallas_call(
        kernel,
        in_specs=[smem] * scalars + [VMEM] * (len(inputs) - scalars),
        out_specs=[VMEM] * len(outputs),
        out_shape=list(outputs),
        compiler_params=pltpu.CompilerParams(vmem_limit_bytes=VMEM_LIMIT),
        cost_estimate=cost(flops, moved),
    )(*inputs)


def shape(dims, dtype=BF16):
    return jax.ShapeDtypeStruct(tuple(dims), dtype)


def block_of(ref, g, h_ref, width):
    return ref[:, pl.ds(pl.multiple_of((2 * g + h_ref[0]) * width, width), width)]


def encode_points(h_ref, xt_refs, val_ref, cond_refs, out_ref, width):
    pieces, _, piece = out_ref.shape
    per_block = width // piece
    cols = min(256, piece)

    def block(g, carry):
        base = pl.multiple_of((2 * g + h_ref[0]) * width, width)
        for first in range(0, width, cols):
            at = pl.ds(pl.multiple_of(base + first, cols), cols)
            val = val_ref[:, at]
            total = jnp.zeros((K, cols), F32)
            for xt_ref, cond_ref in zip(xt_refs, cond_refs):
                cond = cond_ref[:, at].astype(F32)
                for c in range(0, cond.shape[0], 4):
                    part = jnp.dot(xt_ref[c * K : (c + 4) * K, :], val, preferred_element_type=F32)
                    for i in range(4):
                        total = total + part[i * K : (i + 1) * K] * cond[c + i : c + i + 1]
            out_ref[g * per_block + first // piece, :, first % piece : first % piece + cols] = total.astype(BF16)
        return carry

    lax.fori_loop(0, pieces // per_block, block, 0, unroll=UNROLL)


def encode_first(width, h_ref, xt_ref, xt_other_ref, val_ref, cond_ref, cond_other_ref, out_ref):
    encode_points(h_ref, (xt_ref, xt_other_ref), val_ref, (cond_ref, cond_other_ref), out_ref, width)


def stepped(xt, gap, coupled):
    scale = (gap - CENTER) * (1.0 / HALF_WIDTH)
    scale = jnp.broadcast_to(scale[:, None, :], (scale.shape[0], K, scale.shape[1])).reshape(xt.shape)
    return xt.astype(F32) * scale + coupled * (2.0 / HALF_WIDTH)


def encode_next(
    width,
    h_ref,
    part_ref,
    recv_ref,
    old_ref,
    old_other_ref,
    gap_ref,
    gap_other_ref,
    val_ref,
    cond_ref,
    cond_other_ref,
    out_ref,
    xt_ref,
    xt_other_ref,
):
    half = old_ref.shape[0]
    sides = ((old_ref, gap_ref, xt_ref), (old_other_ref, gap_other_ref, xt_other_ref))
    for side, (old, gap, new) in enumerate(sides):
        here = slice(side * half, (side + 1) * half)
        there = slice((1 - side) * half, (2 - side) * half)
        coupled = part_ref[here] + recv_ref[there].astype(F32)
        new[...] = stepped(old[...], gap[...], coupled).astype(BF16)
    encode_points(h_ref, (xt_ref, xt_other_ref), val_ref, (cond_ref, cond_other_ref), out_ref, width)


def encode(kernel, h, whole, orbitals, pieces, piece, width, *more):
    val_count, points = orbitals[0].shape
    rows = orbitals[1].shape[0] * K
    return call(
        functools.partial(kernel, width),
        (h, *whole, *orbitals),
        (shape((pieces, K, piece)), *more),
        2 * rows * val_count * points,
        1,
    )


def total_kernel(in_ref, out_ref):
    total = in_ref[0].astype(F32)
    for index in range(1, in_ref.shape[0]):
        total = total + in_ref[index].astype(F32)
    total = total.astype(BF16)
    for copy in range(out_ref.shape[0]):
        out_ref[copy] = total


def summed(array, copies):
    return call(total_kernel, (array,), (shape((copies, *array.shape[1:])),), array.size)[0]


def apply_kernel(pieces, width, h_ref, own_ref, other_ref, kernel_ref, out_ref):
    piece = own_ref.shape[2]
    even = h_ref[0] == 0

    def added(ref, q):
        shares = ref.shape[0] // pieces
        total = ref[q * shares].astype(F32)
        for index in range(q * shares + 1, (q + 1) * shares):
            total = total + ref[index].astype(F32)
        return total

    total = jnp.zeros((K, kernel_ref.shape[0]), F32)
    for q in range(pieces):
        own, other = added(own_ref, q), added(other_ref, q)
        for side in range(2):
            fit = jnp.where(even, own, other) if side == 0 else jnp.where(even, other, own)
            at = q * piece
            first = width * (2 * (at // width) + side) + at % width
            total = total + lax.dot_general(
                fit.astype(BF16),
                kernel_ref[:, first : first + piece],
                (((1,), (1,)), ((), ())),
                preferred_element_type=F32,
            )
    total = total.astype(BF16)
    for copy in range(out_ref.shape[0]):
        out_ref[copy] = total


def applied(h, own, other, kernel, pieces, copies):
    rows = kernel.shape[0]
    return call(
        functools.partial(apply_kernel, pieces, rows),
        (h, own, other, kernel),
        (shape((copies, K, rows)),),
        2 * K * kernel.size,
        1,
    )[0]


def stack_kernel(*refs):
    out_ref = refs[-1]
    for index, ref in enumerate(refs[:-1]):
        out_ref[index] = ref[0]


def stacked(arrays):
    return call(stack_kernel, arrays, (shape((len(arrays), *arrays[0].shape[1:])),), arrays[0].size)[0]


def decode_kernel(steps, sizes, more, h_ref, zh_ref, y_ref, field_ref, val_ref, cond_ref, cond_other_ref, *refs):
    before = refs[:more]
    part_ref, send_ref = (*refs[more:], None)[:2]
    width = field_ref.shape[2]
    for index, z_step in enumerate(steps):
        g = lax.rem(zh_ref[0] + sizes["zh"] - z_step, sizes["zh"]) * sizes["y"] + y_ref[0]
        field = field_ref[index].astype(F32)
        val = block_of(val_ref, g, h_ref, width)
        row = 0
        for ref in (cond_ref, cond_other_ref):
            cond = block_of(ref, g, h_ref, width).astype(F32)
            for c in range(0, cond.shape[0], 4):
                pairs = jnp.concatenate([cond[c + i : c + i + 1] * field for i in range(4)], 0).astype(BF16)
                rows = slice(row, row + 4 * K)
                added = lax.dot_general(pairs, val, (((1,), (1,)), ((), ())), preferred_element_type=F32)
                if index == 0:
                    part_ref[rows, :] = before[0][rows, :] + added if before else added
                else:
                    part_ref[rows, :] += added
                row += 4 * K
    if send_ref is not None:
        send_ref[...] = part_ref[part_ref.shape[0] - send_ref.shape[0] :].astype(BF16)


def behind(count):
    return sorted(range(1, count), key=lambda step: -min(step, count - step))


def shifted(array, axis, count, step):
    return lax.ppermute(array, axis, [(i, (i + step) % count) for i in range(count)])


def decode(field, place, orbitals, sizes, sent):
    val_count = orbitals[0].shape[0]
    rows = 2 * orbitals[1].shape[0] * K
    steps = [0, *behind(sizes["zh"])]
    fields = [field]
    for step in steps[1:]:
        fields.append(shifted(field, "zh", sizes["zh"], step))
    field = stacked(fields)
    far = behind(sizes["y"])
    fields = {step: shifted(field, "y", sizes["y"], step) for step in far}
    fields[0] = field
    h, zh, y = place
    parts = ()
    for y_step in (0, *reversed(far)):
        here = fields[y_step]
        outputs = (shape((rows, val_count), F32),)
        if y_step == far[0]:
            outputs += (shape((sent, val_count)),)
        parts = call(
            functools.partial(decode_kernel, tuple(steps), sizes, len(parts)),
            (h, zh, lax.rem(y + (sizes["y"] - y_step), sizes["y"]), here, *orbitals, *parts),
            outputs,
            2 * rows * val_count * here.shape[0] * here.shape[2],
            len(place),
        )
    return parts


def turn_kernel(xt_ref, out_ref):
    out_ref[...] = xt_ref[...].astype(F32).T.astype(BF16)


def turned(xt, flops):
    return call(turn_kernel, (xt,), (shape(xt.shape[::-1]),), flops)[0]


def finish_kernel(part_ref, recv_ref, xt_ref, gap_ref, trial_ref, out_ref):
    rows = recv_ref.shape[0]
    coupled = part_ref[:rows] + recv_ref[...].astype(F32)
    second = stepped(xt_ref[...], gap_ref[...], coupled)
    out_ref[...] = (2.0 * second.T - trial_ref[...].astype(F32)).astype(BF16)


def finish(part, recv, xt, gap, trial):
    return call(finish_kernel, (part, recv, xt, gap, trial), (shape(trial.shape),), 8 * trial.size)[0]


def field_of(encoded, h, kernel, sizes):
    ring = sizes["zh"] * sizes["y"]
    shares = exchange(encoded, (*VAL, "y"))
    shares = exchange(summed(shares, ring), RING)
    image = applied(h, shares, swap_cores(shares), kernel, sizes["y"], sizes["x"] * sizes["zl"])
    return summed(exchange(image, VAL), 1)


def on_device(sizes, trial, energy_gap, orb_val, orb_cond, kernel):
    width = kernel.shape[0]
    pieces = sizes["x"] * sizes["zl"] * sizes["y"]
    piece = kernel.shape[1] // 2 // sizes["y"]
    place = [lax.axis_index(axis).astype(jnp.int32).reshape(1) for axis in ("core", "zh", "y")]
    h = place[0]
    orbitals = (orb_val, orb_cond, swap_cores(orb_cond))
    gap = energy_gap.T
    xt = turned(trial, START_FLOPS)
    xt_other = swap_cores(xt)

    encoded = encode(encode_first, h, (xt, xt_other), orbitals, pieces, piece, width)[0]
    field = field_of(encoded, h, kernel, sizes)
    part, sent = decode(field, place, orbitals, sizes, 2 * xt.shape[0])
    whole = (part, swap_cores(sent), xt, xt_other, gap, swap_cores(gap))
    states = (shape(xt.shape), shape(xt.shape))
    encoded, xt, _ = encode(encode_next, h, whole, orbitals, pieces, piece, width, *states)
    first_step = turned(xt, xt.size)
    field = field_of(encoded, h, kernel, sizes)
    part, sent = decode(field, place, orbitals, sizes, xt.shape[0])
    filtered = finish(part, swap_cores(sent), xt, gap, trial)
    return first_step, filtered


def build(mesh, fine):
    split = Mesh(mesh.devices.reshape([size for _, size in fine]), [name for name, _ in fine])
    placed = (P(VAL, PTS), P(VAL, PTS), P(VAL, None), P(PTS, None), P(PTS, VAL))
    return jax.shard_map(
        functools.partial(on_device, dict(fine)),
        mesh=split,
        in_specs=placed,
        out_specs=(P(VAL, PTS), P(VAL, PTS)),
        check_vma=False,
    )


def solution(mesh):
    return build(mesh, FINE)
```
